32 devices in a mesh: section: 16 (over z, y, core), tensor: 2 (over x).
Axes of the slice: x: 2, y: 2, z: 4, core: 2. Of those that a mesh axis runs over, the one named last changes fastest.
Arguments:
- saved: bfloat16 [16, 16, 64, 8192], P('section', None, 'tensor'), may hold values from -6 to 6
- offsets: int32 [16, 16], P('section'), may hold values from 0 to 15, as said below
Outputs:
- restored: float32 [16, 16, 64, 8192], P('section', None, None, 'tensor')
- block_sums: float32 [16, 16, 8192], P('section', None, 'tensor')
The draws below stay inside these ranges and needn't reach their ends.
Inputs may be any that keep to these rules, and one draw needn't show every extreme that they name: Each row of offsets is a permutation of 0 to 15.
All inputs are finite; a program needn't handle non-finite values.
Results may differ from the reference program's by a relative error of at most 0.0003.
Values may be sent and summed in bfloat16 or wider, within the bound.
A program may use at most 128 MiB of HBM per device.

```python
import jax
import jax.numpy as jnp

D = 8192
R = 64
SLOTS = 16
N_SECTION = 16


def draw_offsets(key, part):
    row_keys = jax.random.split(jax.random.fold_in(key, 17), N_SECTION)
    rows = jax.vmap(lambda k: jax.random.permutation(k, N_SECTION))(row_keys)
    return rows.astype(jnp.int32)


def shard_levels(stream_key, dims, cuts, least, largest):
    def one(dim, parts):
        draws = jax.random.uniform(jax.random.fold_in(jax.random.fold_in(stream_key, 6), dim), (parts,), jnp.float32, least / len(cuts), largest / len(cuts))
        return jnp.repeat(jnp.exp(draws), dims[dim] // parts).reshape((-1,) + (1,) * (len(dims) - dim - 1))

    factor_of = one(*cuts[0])
    for cut in cuts[1:]:
        factor_of = factor_of * one(*cut)
    return factor_of


def gaussian(stream_key, dims, width, limit, cuts=(), kind=jnp.bfloat16):
    loudness = shard_levels(stream_key, dims, cuts, -0.22, 0.18) if cuts else 1.0
    entries = jax.random.normal(stream_key, dims, jnp.float32) * width * loudness
    return jnp.minimum(jnp.maximum(entries, -limit), limit).astype(kind)


def setup_inputs(seed: int = 0) -> dict:
    keys = jax.random.split(jax.random.key(seed), 3)
    return {
        "saved": gaussian(keys[0], (N_SECTION, SLOTS, R, D), 1.0, 6.0, ((0, 16), (2, 2))),
        "offsets": draw_offsets(jax.random.fold_in(keys[2], 71), 0),
    }


def reference(saved, offsets):
    sections = jnp.arange(N_SECTION, dtype=jnp.int32)
    relative = ((sections[:, None] - sections[None, :]) % N_SECTION).astype(jnp.int32)
    inverse = jnp.argsort(offsets, axis=1).astype(jnp.int32)
    sources = jnp.broadcast_to(sections[None, :], (N_SECTION, N_SECTION)).astype(jnp.int32)
    chosen = inverse[sources, relative]
    blocks = saved[sources, chosen]
    restored = blocks.astype(jnp.float32)
    block_sums = jnp.sum(restored, axis=2)
    return restored, block_sums
```

```python
import jax
import jax.numpy as jnp
from jax import lax
from jax.experimental import pallas as pl
from jax.experimental.pallas import tpu as pltpu
from jax.sharding import PartitionSpec as P

MESH = pl.DeviceIdType.MESH


def partner(index, step, count):
    if count & (count - 1):
        return (index + step) % count
    other = index
    bit = 1
    while bit < count:
        if step & bit:
            other = other + bit * (1 - 2 * ((index // bit) % 2))
        bit *= 2
    return other


def send_order(n, m):
    far = [(k, e) for k in range(n // 2, n) for e in range(m)]
    near = [(k, e) for k in range(n // 2 - 1, -1, -1) for e in range(m)]
    mixed = []
    for i in range(max(len(far), len(near))):
        mixed += far[i : i + 1] + near[i : i + 1]
    return mixed


def exchange(n, m, offsets, saved, arrived, held, out_box, load_sem, send_sem, recv_sem, own_sem):
    s = lax.axis_index("section")
    x = lax.axis_index("tensor")
    rows = saved.shape[1]
    cols = saved.shape[2] // m
    load = pltpu.make_async_copy(saved, held, load_sem)
    load.start()

    barrier = pltpu.get_barrier_semaphore()

    def greet(i, carry):
        j = i + 1
        pl.semaphore_signal(
            barrier,
            inc=1,
            device_id=((s + j // m) % n, (x + j % m) % m),
            device_id_type=MESH,
        )
        return carry

    lax.fori_loop(0, n * m - 1, greet, 0)
    load.wait()
    greeted = [False]

    def send(k, e):
        t = partner(s, k, n)
        d = partner(x, e, m)
        dst = arrived.at[s, pl.ds(x * rows, rows), :]
        if k == 0 and e == 0:
            return pltpu.make_async_copy(out_box.at[0], dst, own_sem)
        return pltpu.make_async_remote_copy(
            src_ref=out_box.at[k * m + e],
            dst_ref=dst,
            send_sem=send_sem.at[k * m + e],
            recv_sem=recv_sem.at[k * m + e],
            device_id=(t, d),
            device_id_type=MESH,
        )

    def fill(k, e):
        t = partner(s, k, n)
        d = partner(x, e, m)
        wanted = (t - s + n) % n
        slot = jnp.int32(0)
        for j in range(n):
            slot = jnp.where(offsets[0, j] == wanted, jnp.int32(j), slot)
        step = min(cols, 512)

        def move(i, carry):
            src = pl.ds(pl.multiple_of(d * cols + i * step, step), step)
            dst = pl.ds(pl.multiple_of(i * step, step), step)
            out_box[k * m + e, :, dst] = held[slot, :, src]
            return carry

        lax.fori_loop(0, cols // step, move, 0)

    copies = []
    waiting = None
    for k, e in send_order(n, m):
        fill(k, e)
        if waiting is not None:
            if not copies:
                pl.semaphore_wait(barrier, n * m - 1)
            copy = send(*waiting)
            copy.start()
            copies.append(copy)
        waiting = (k, e)
    copy = send(*waiting)
    copy.start()
    copies.append(copy)
    for copy in copies:
        copy.wait()


def body(n, m, saved, offsets):
    _, slots, rows, width = saved.shape
    cols = width // m
    arrived = pl.pallas_call(
        lambda *refs: exchange(n, m, *refs),
        out_shape=jax.ShapeDtypeStruct((slots, rows * m, cols), saved.dtype),
        in_specs=[
            pl.BlockSpec(memory_space=pltpu.SMEM),
            pl.BlockSpec(memory_space=pl.ANY),
        ],
        out_specs=pl.BlockSpec(memory_space=pl.ANY),
        scratch_shapes=[
            pltpu.VMEM((slots, rows, width), saved.dtype),
            pltpu.VMEM((slots * m, rows, cols), saved.dtype),
            pltpu.SemaphoreType.DMA,
            pltpu.SemaphoreType.DMA((n * m,)),
            pltpu.SemaphoreType.DMA((n * m,)),
            pltpu.SemaphoreType.DMA,
        ],
        compiler_params=pltpu.CompilerParams(
            collective_id=0, has_side_effects=True, vmem_limit_bytes=48 * 2**20
        ),
        name="exchange",
    )(offsets, saved[0])
    restored = arrived.astype(jnp.float32)
    block_sums = jnp.sum(restored, axis=1)
    return (restored[None], block_sums[None])


def solution(mesh):
    n = mesh.shape["section"]
    m = mesh.shape["tensor"]
    return jax.shard_map(
        lambda saved, offsets: body(n, m, saved, offsets),
        mesh=mesh,
        in_specs=(P("section", None, "tensor", None), P("section", None)),
        out_specs=(P("section", None, None, "tensor"), P("section", None, "tensor")),
        check_vma=False,
    )
```

```python
import jax
import jax.numpy as jnp
from jax import lax
from jax.experimental import pallas as pl
from jax.experimental.pallas import tpu as pltpu
from jax.sharding import PartitionSpec as P

MESH = pl.DeviceIdType.MESH


def partner(index, step, count):
    if count & (count - 1):
        return (index + step) % count
    other = index
    bit = 1
    while bit < count:
        if step & bit:
            other = other + bit * (1 - 2 * ((index // bit) % 2))
        bit *= 2
    return other


def send_order(n, m):
    far = [(k, e) for k in range(n // 2, n) for e in range(m)]
    near = [(k, e) for k in range(n // 2 - 1, -1, -1) for e in range(m)]
    mixed = []
    for i in range(max(len(far), len(near))):
        mixed += far[i : i + 1] + near[i : i + 1]
    return mixed


def exchange(n, m, offsets, saved, arrived, held, out_box, load_sem, send_sem, recv_sem, own_sem):
    s = lax.axis_index("section")
    x = lax.axis_index("tensor")
    rows = saved.shape[1]
    cols = saved.shape[2] // m
    load = pltpu.make_async_copy(saved, held, load_sem)
    load.start()

    barrier = pltpu.get_barrier_semaphore()

    def greet(i, carry):
        j = i + 1
        pl.semaphore_signal(
            barrier,
            inc=1,
            device_id=((s + j // m) % n, (x + j % m) % m),
            device_id_type=MESH,
        )
        return carry

    lax.fori_loop(0, n * m - 1, greet, 0)
    load.wait()
    greeted = [False]

    def send(k, e):
        t = partner(s, k, n)
        d = partner(x, e, m)
        dst = arrived.at[s, pl.ds(x * rows, rows), :]
        if k == 0 and e == 0:
            return pltpu.make_async_copy(out_box.at[0], dst, own_sem)
        return pltpu.make_async_remote_copy(
            src_ref=out_box.at[k * m + e],
            dst_ref=dst,
            send_sem=send_sem.at[k * m + e],
            recv_sem=recv_sem.at[k * m + e],
            device_id=(t, d),
            device_id_type=MESH,
        )

    def fill(k, e):
        t = partner(s, k, n)
        d = partner(x, e, m)
        wanted = (t - s + n) % n
        slot = jnp.int32(0)
        for j in range(n):
            slot = jnp.where(offsets[0, j] == wanted, jnp.int32(j), slot)
        step = min(cols, 512)

        def move(i, carry):
            src = pl.ds(pl.multiple_of(d * cols + i * step, step), step)
            dst = pl.ds(pl.multiple_of(i * step, step), step)
            out_box[k * m + e, :, dst] = held[slot, :, src]
            return carry

        lax.fori_loop(0, cols // step, move, 0)

    copies = []
    waiting = None
    for k, e in send_order(n, m):
        fill(k, e)
        if waiting is not None:
            if not copies:
                pl.semaphore_wait(barrier, n * m - 1)
            copy = send(*waiting)
            copy.start()
            copies.append(copy)
        waiting = (k, e)
    copy = send(*waiting)
    copy.start()
    copies.append(copy)
    for copy in copies:
        copy.wait()


def widen(arrived, restored, sums):
    i = pl.program_id(0)
    rows, cols = arrived.shape[1:]
    wide = min(cols, 512)
    for c in range(0, cols, wide):
        here = pl.ds(c, wide)
        total = None
        for r in range(0, rows, 16):
            band = pl.ds(r, min(16, rows - r))
            part = arrived[i, band, here].astype(jnp.float32)
            restored[0, band, here] = part
            total = part if total is None else total + part
        sums[pl.ds(i, 1), here] = jnp.sum(total, axis=0, keepdims=True)


def body(n, m, saved, offsets):
    _, slots, rows, width = saved.shape
    cols = width // m
    arrived = pl.pallas_call(
        lambda *refs: exchange(n, m, *refs),
        out_shape=jax.ShapeDtypeStruct((slots, rows * m, cols), saved.dtype),
        in_specs=[
            pl.BlockSpec(memory_space=pltpu.SMEM),
            pl.BlockSpec(memory_space=pltpu.HBM),
        ],
        out_specs=pl.BlockSpec(memory_space=pl.ANY),
        scratch_shapes=[
            pltpu.VMEM((slots, rows, width), saved.dtype),
            pltpu.VMEM((slots * m, rows, cols), saved.dtype),
            pltpu.SemaphoreType.DMA,
            pltpu.SemaphoreType.DMA((n * m,)),
            pltpu.SemaphoreType.DMA((n * m,)),
            pltpu.SemaphoreType.DMA,
        ],
        compiler_params=pltpu.CompilerParams(
            collective_id=0, has_side_effects=True, vmem_limit_bytes=20 * 2**20
        ),
        name="exchange",
    )(offsets, pltpu.with_memory_space_constraint(saved[0], pltpu.HBM))
    blocks, height = arrived.shape[:2]
    restored, block_sums = pl.pallas_call(
        widen,
        grid=(blocks,),
        out_shape=[
            jax.ShapeDtypeStruct(arrived.shape, jnp.float32),
            jax.ShapeDtypeStruct((blocks, cols), jnp.float32),
        ],
        in_specs=[pl.BlockSpec(memory_space=pltpu.VMEM)],
        out_specs=[
            pl.BlockSpec((1, height, cols), lambda i: (i, 0, 0)),
            pl.BlockSpec((blocks, cols), lambda i: (0, 0)),
        ],
        compiler_params=pltpu.CompilerParams(vmem_limit_bytes=16 * 2**20),
        name="widen",
    )(arrived)
    return (restored[None], block_sums[None])


def solution(mesh):
    n = mesh.shape["section"]
    m = mesh.shape["tensor"]
    return jax.shard_map(
        lambda saved, offsets: body(n, m, saved, offsets),
        mesh=mesh,
        in_specs=(P("section", None, "tensor", None), P("section", None)),
        out_specs=(P("section", None, None, "tensor"), P("section", None, "tensor")),
        check_vma=False,
    )
```

```python
import jax
import jax.numpy as jnp
from jax import lax
from jax.experimental import pallas as pl
from jax.experimental.pallas import tpu as pltpu
from jax.sharding import PartitionSpec as P

MESH = pl.DeviceIdType.MESH


def partner(index, step, count):
    if count & (count - 1):
        return (index + step) % count
    other = index
    bit = 1
    while bit < count:
        if step & bit:
            other = other + bit * (1 - 2 * ((index // bit) % 2))
        bit *= 2
    return other


def send_order(n, m):
    far = [(k, e) for k in range(n // 2, n) for e in range(m)]
    near = [(k, e) for k in range(n // 2 - 1, -1, -1) for e in range(m)]
    mixed = []
    for i in range(max(len(far), len(near))):
        mixed += far[i : i + 1] + near[i : i + 1]
    return mixed


def exchange(n, m, offsets, saved, arrived, held, out_box, load_sem, send_sem, recv_sem, own_sem):
    s = lax.axis_index("section")
    x = lax.axis_index("tensor")
    rows = saved.shape[1]
    cols = saved.shape[2] // m
    load = pltpu.make_async_copy(saved, held, load_sem)
    load.start()

    barrier = pltpu.get_barrier_semaphore()

    def greet(i, carry):
        j = i + 1
        pl.semaphore_signal(
            barrier,
            inc=1,
            device_id=((s + j // m) % n, (x + j % m) % m),
            device_id_type=MESH,
        )
        return carry

    lax.fori_loop(0, n * m - 1, greet, 0)
    load.wait()
    greeted = [False]

    def send(k, e):
        t = partner(s, k, n)
        d = partner(x, e, m)
        dst = arrived.at[s, pl.ds(x * rows, rows), :]
        if k == 0 and e == 0:
            return pltpu.make_async_copy(out_box.at[0], dst, own_sem)
        return pltpu.make_async_remote_copy(
            src_ref=out_box.at[k * m + e],
            dst_ref=dst,
            send_sem=send_sem.at[k * m + e],
            recv_sem=recv_sem.at[k * m + e],
            device_id=(t, d),
            device_id_type=MESH,
        )

    def fill(k, e):
        t = partner(s, k, n)
        d = partner(x, e, m)
        wanted = (t - s + n) % n
        slot = jnp.int32(0)
        for j in range(n):
            slot = jnp.where(offsets[0, j] == wanted, jnp.int32(j), slot)
        step = min(cols, 512)

        def move(i, carry):
            src = pl.ds(pl.multiple_of(d * cols + i * step, step), step)
            dst = pl.ds(pl.multiple_of(i * step, step), step)
            out_box[k * m + e, :, dst] = held[slot, :, src]
            return carry

        lax.fori_loop(0, cols // step, move, 0)

    copies = []
    waiting = None
    for k, e in send_order(n, m):
        fill(k, e)
        if waiting is not None:
            if not copies:
                pl.semaphore_wait(barrier, n * m - 1)
            copy = send(*waiting)
            copy.start()
            copies.append(copy)
        waiting = (k, e)
    copy = send(*waiting)
    copy.start()
    copies.append(copy)
    for copy in copies:
        copy.wait()


def widen(arrived, restored, sums, stage, stage_sem):
    blocks, rows, cols = arrived.shape
    depth = stage.shape[0]
    wide = min(cols, 512)
    copies = []
    for i in range(blocks):
        slot = i % depth
        if i >= depth:
            copies[i - depth].wait()
        for c in range(0, cols, wide):
            here = pl.ds(c, wide)
            total = None
            for r in range(0, rows, 16):
                band = pl.ds(r, min(16, rows - r))
                part = arrived[i, band, here].astype(jnp.float32)
                stage[slot, band, here] = part
                total = part if total is None else total + part
            sums[pl.ds(i, 1), here] = jnp.sum(total, axis=0, keepdims=True)
        copy = pltpu.make_async_copy(stage.at[slot], restored.at[i], stage_sem.at[slot])
        copy.start()
        copies.append(copy)
    for copy in copies[-depth:]:
        copy.wait()


def body(n, m, saved, offsets):
    _, slots, rows, width = saved.shape
    cols = width // m
    arrived = pl.pallas_call(
        lambda *refs: exchange(n, m, *refs),
        out_shape=jax.ShapeDtypeStruct((slots, rows * m, cols), saved.dtype),
        in_specs=[
            pl.BlockSpec(memory_space=pltpu.SMEM),
            pl.BlockSpec(memory_space=pltpu.HBM),
        ],
        out_specs=pl.BlockSpec(memory_space=pl.ANY),
        scratch_shapes=[
            pltpu.VMEM((slots, rows, width), saved.dtype),
            pltpu.VMEM((slots * m, rows, cols), saved.dtype),
            pltpu.SemaphoreType.DMA,
            pltpu.SemaphoreType.DMA((n * m,)),
            pltpu.SemaphoreType.DMA((n * m,)),
            pltpu.SemaphoreType.DMA,
        ],
        compiler_params=pltpu.CompilerParams(
            collective_id=0, has_side_effects=True, vmem_limit_bytes=20 * 2**20
        ),
        name="exchange",
    )(offsets, pltpu.with_memory_space_constraint(saved[0], pltpu.HBM))
    blocks, height = arrived.shape[:2]
    restored, block_sums = pl.pallas_call(
        widen,
        out_shape=[
            jax.ShapeDtypeStruct(arrived.shape, jnp.float32),
            jax.ShapeDtypeStruct((blocks, cols), jnp.float32),
        ],
        in_specs=[pl.BlockSpec(memory_space=pltpu.VMEM)],
        out_specs=[
            pl.BlockSpec(memory_space=pl.ANY),
            pl.BlockSpec(memory_space=pltpu.VMEM),
        ],
        scratch_shapes=[
            pltpu.VMEM((6, height, cols), jnp.float32),
            pltpu.SemaphoreType.DMA((6,)),
        ],
        compiler_params=pltpu.CompilerParams(vmem_limit_bytes=20 * 2**20),
        name="widen",
    )(arrived)
    return (restored[None], block_sums[None])


def solution(mesh):
    n = mesh.shape["section"]
    m = mesh.shape["tensor"]
    return jax.shard_map(
        lambda saved, offsets: body(n, m, saved, offsets),
        mesh=mesh,
        in_specs=(P("section", None, "tensor", None), P("section", None)),
        out_specs=(P("section", None, None, "tensor"), P("section", None, "tensor")),
        check_vma=False,
    )
```
